128 devices in a mesh: slab: 64 (over y, z_lo, x, core), grp: 2 (over z_hi).
Axes of the slice: x: 4, y: 4, z: 4 (z_hi: 2, z_lo: 2; z = z_hi * 2 + z_lo), core: 2. Of those that a mesh axis runs over, the one named last changes fastest.
Arguments:
- capture: float32 [2, 1048576], P(None, ('slab', 'grp')), may hold values from -6 to 6
- dropped: int32 [64], P('slab'), may hold values from 0 to 8191
Outputs:
- max_held: float32 [128, 128, 128], P('slab', 'grp')
- coherent: float32 [2, 128, 128, 128], P(None, 'slab', 'grp')
The draws below stay inside these ranges and needn't reach their ends.
All inputs are finite; a program needn't handle non-finite values.
Results may differ from the reference program's by a relative error of at most 0.0001.
Values sent between devices are 32-bit elements; how exact they have to be, the bound alone decides.
A program may use at most 128 MiB of HBM per device.

```python
import math
import jax
import jax.numpy as jnp
from jax import lax

NCH = 256
HOP = 64
KW = 128
LW = 128
Q = 128
BLOCKS = 2
SAMPLES = 1048576
N_SLAB = 64


def set_ends(values, own_key, smallest, top_value):
    shape = values.shape
    place = [jax.random.randint(jax.random.fold_in(own_key, axis), (), 0, shape[axis]) for axis in range(len(shape))]
    values = values.at[tuple(place)].set(smallest)
    longest = shape.index(max(shape))
    place[longest] = (place[longest] + 1) % shape[longest]
    return values.at[tuple(place)].set(top_value)


def steps_of(rng, extent, pieces, low, high):
    def one(position, parts):
        draws = jax.random.uniform(jax.random.fold_in(jax.random.fold_in(rng, 6), position), (parts,), jnp.float32, low / len(pieces), high / len(pieces))
        return jnp.repeat(jnp.exp(draws), extent[position] // parts).reshape((-1,) + (1,) * (len(extent) - position - 1))

    loudness = one(*pieces[0])
    for cut in pieces[1:]:
        loudness = loudness * one(*cut)
    return loudness


def gaussian(rng, dims, scale, bound, pieces=(), kind=jnp.bfloat16):
    loudness = steps_of(rng, dims, pieces, -0.22, 0.18) if pieces else 1.0
    array = jax.random.normal(rng, dims, jnp.float32) * scale * loudness
    return jnp.minimum(jnp.maximum(array, -bound), bound).astype(kind)


def setup_inputs(seed: int = 0) -> dict:
    streams_of = jax.random.split(jax.random.key(seed), 3)
    return {
        "capture": gaussian(streams_of[0], (2, SAMPLES), 1.0, 6.0, ((1, 128),), jnp.float32),
        "dropped": set_ends(jax.random.randint(streams_of[1], (N_SLAB,), 0, Q * HOP), jax.random.fold_in(streams_of[1], 1), 0, (Q * HOP) - 1).astype(jnp.int32),
    }


def reference(capture, dropped):
    lead_hops = NCH // HOP - 1
    slab_hops = BLOCKS * Q
    total_hops = N_SLAB * slab_hops
    padded = jnp.concatenate([jnp.zeros((2, lead_hops * HOP), capture.dtype), capture], axis=1)
    hop_rows = padded.reshape(2, total_hops + lead_hops, HOP)
    frames = jnp.concatenate([hop_rows[:, lag_index:lag_index + total_hops] for lag_index in range(lead_hops + 1)], axis=2)
    tap_index = jnp.arange(NCH, dtype=jnp.int32).astype(jnp.float32)
    window = 0.5 - 0.5 * jnp.cos(2.0 * math.pi * tap_index / NCH)
    scaling = 1.0 / jnp.sqrt(jnp.sum(window * window))
    signal = lax.complex(frames[0] * window, frames[1] * window)
    spectra = jnp.fft.fft(signal, axis=-1)[:, :KW + LW] * scaling
    stamps = jnp.arange(N_SLAB, dtype=jnp.int32) * (BLOCKS * Q * HOP) + jnp.cumsum(dropped).astype(jnp.int32)
    hop_start = jnp.arange(slab_hops, dtype=jnp.int32) * HOP
    clock_mod = ((stamps[:, None] % NCH + hop_start[None, :]) % NCH).reshape(total_hops)
    channels = jnp.arange(KW + LW, dtype=jnp.int32)
    chan_turns = (clock_mod[:, None] * channels[None, :] % NCH).astype(jnp.float32) * (2.0 * math.pi / NCH)
    shifted = spectra * lax.complex(jnp.cos(chan_turns), -jnp.sin(chan_turns))
    shifted = shifted.reshape(N_SLAB, BLOCKS, Q, KW + LW)
    clock_period = Q * HOP
    freq_bins = jnp.arange(Q, dtype=jnp.int32)
    cycle_turns = (freq_bins[None, :] * (stamps % clock_period)[:, None] % clock_period).astype(jnp.float32) * (2.0 * math.pi / clock_period)
    rotation = lax.complex(jnp.cos(cycle_turns), -jnp.sin(cycle_turns))

    def accumulate(state_pair, slab_item):
        largest, running = state_pair
        slab_spectra, slab_rotation = slab_item
        lower_bank = slab_spectra[:, :, :KW]
        upper_bank = slab_spectra[:, :, KW:]
        products = lower_bank[:, :, :, None] * jnp.conj(upper_bank)[:, :, None, :]
        surfaces = jnp.fft.fft(products, axis=1) / math.sqrt(Q)
        largest = jnp.maximum(largest, lax.optimization_barrier(jnp.max(jnp.abs(surfaces), axis=0)))
        running = running + slab_rotation[:, None, None] * lax.optimization_barrier(jnp.sum(surfaces, axis=0))
        return ((largest, running), None)
    empty_surface = jnp.zeros((Q, KW, LW), jnp.float32)
    (largest, running), unused = lax.scan(accumulate, (empty_surface, lax.complex(empty_surface, empty_surface)), (shifted, rotation))
    norm_scale = 1.0 / math.sqrt(N_SLAB * BLOCKS)
    coherent = jnp.stack([jnp.real(running), jnp.imag(running)]) * norm_scale
    return (largest, coherent)
```

```python
import math

import jax
import jax.numpy as jnp
import numpy as np
from jax import lax
from jax.experimental import pallas as pl
from jax.experimental.pallas import tpu as pltpu
from jax.sharding import Mesh, PartitionSpec as P

NCH = 256
HOP = 64
Q = 128
PERIOD = Q * HOP
AXES = ("y", "zl", "x", "c", "zh")
MESH = pl.DeviceIdType.MESH
F32 = jnp.float32
BF16 = jnp.bfloat16


def tables():
    tap = np.arange(NCH)
    window = 0.5 - 0.5 * np.cos(2.0 * np.pi * tap / NCH)
    window = window / np.sqrt(np.sum(window * window))
    win = np.zeros((8, NCH), np.float32)
    for r in range(4):
        win[r] = window[(tap - 64 * (r + 1)) % NCH]
    turns = ((tap[:, None] + 192) * tap[None, :]) % NCH
    cos = np.cos(2.0 * np.pi * turns / NCH)
    sin = np.sin(2.0 * np.pi * turns / NCH)
    real = np.concatenate([cos, sin], axis=0)
    imag = np.concatenate([-sin, cos], axis=0)
    parts = []
    for lo in (0, 64):
        parts.append(np.concatenate([real[:, lo : lo + 64], imag[:, lo : lo + 64]], axis=1))
    parts.append(real[:, 128:])
    parts.append(imag[:, 128:])
    full = np.stack(parts).astype(np.float32)
    high = full.astype(jnp.bfloat16)
    low = (full - high.astype(np.float32)).astype(jnp.bfloat16)
    return win, np.stack([high, low])


def split(value):
    high = value.astype(BF16)
    return high, (value - high.astype(F32)).astype(BF16)


def kernel(
    cap, meta_in, win, w_hbm, out_max, out_coh,
    pay, xs, wscr, ysc, at, wb, etab, ltab, ktab, mteam, mplane, acc_p, acc_o, rec_p, rec_y,
    w_sem, mar_s, mar_r, mt_s, mt_r, mp_s, mp_r, g1_s, g1_r, g2_s, g2_r, d_s, d_r, y_s, y_r,
):
    y = lax.axis_index("y")
    zl = lax.axis_index("zl")
    x = lax.axis_index("x")
    c = lax.axis_index("c")
    zh = lax.axis_index("zh")
    z = zh * 2 + zl

    def dev(yy, xx, zz, cc):
        return {"y": yy, "zl": zz % 2, "x": xx, "c": cc, "zh": zz // 2}

    def block_dev(number):
        s = number // 2
        return {"y": s // 16, "zl": (s // 8) % 2, "x": (s // 2) % 4, "c": s % 2, "zh": number % 2}

    number = (((y * 2 + zl) * 4 + x) * 2 + c) * 2 + zh
    following = block_dev((number + 1) % 128)
    preceding = block_dev((number + 127) % 128)
    team = [(dy, dc) for dy in range(4) for dc in range(2) if (dy, dc) != (0, 0)]
    plane = [(dx, dz) for dx in range(4) for dz in range(4) if (dx, dz) != (0, 0)]

    def team_dev(dy, dc):
        return dev((y + dy) % 4, x, z, (c + dc) % 2)

    def plane_dev(dx, dz):
        return dev(y, (x + dx) % 4, (z + dz) % 4, c)

    def copy(src, dst, send, recv, device):
        return pltpu.make_async_remote_copy(
            src_ref=src, dst_ref=dst, send_sem=send, recv_sem=recv, device_id=device,
            device_id_type=MESH,
        )

    w_copies = []
    for part, which in enumerate((0, 0, 1)):
        rows = pl.ds(part * 512, 512)
        for col, src in enumerate((zh, 2, 3)):
            w_copies.append(
                pltpu.make_async_copy(
                    w_hbm.at[which, src], wscr.at[rows, pl.ds(col * 128, 128)],
                    w_sem.at[part, col],
                )
            )
    for cp in w_copies:
        cp.start()

    barrier = pltpu.get_barrier_semaphore()
    for d in team:
        pl.semaphore_signal(barrier, inc=1, device_id=team_dev(*d), device_id_type=MESH)
    for d in plane:
        pl.semaphore_signal(barrier, inc=1, device_id=plane_dev(*d), device_id_type=MESH)
    pl.semaphore_signal(barrier, inc=1, device_id=following, device_id_type=MESH)
    pl.semaphore_signal(barrier, inc=1, device_id=preceding, device_id_type=MESH)
    own = x * 4 + z
    pay[own, :, 8:40, :] = cap[...]
    pl.semaphore_wait(barrier, len(team) + len(plane) + 2)

    margin = copy(
        cap.at[:, pl.ds(24, 8), :], pay.at[own_slot(following), :, pl.ds(0, 8), :], mar_s, mar_r,
        following,
    )
    margin.start()
    team_copies = []
    for i, d in enumerate(team):
        cp = copy(meta_in, mteam.at[i], mt_s.at[i], mt_r.at[i], team_dev(*d))
        cp.start()
        team_copies.append(cp)
    mplane_own = mplane.at[15]
    for cp in team_copies:
        cp.wait_recv()
    total = meta_in[...]
    for i in range(len(team)):
        total = total + mteam[i]
    mplane_own[...] = total
    margin.wait_recv()

    first = []
    for d in range(1, 4):
        cp = copy(
            pay.at[own], pay.at[own], g1_s.at[d - 1], g1_r.at[d - 1],
            plane_dev(d * (1 - c), d * c),
        )
        cp.start()
        first.append(cp)

    def slot(fd, gd):
        sx = (x + 4 - fd * (1 - c) - gd * c) % 4
        sz = (z + 4 - fd * c - gd * (1 - c)) % 4
        return sx * 4 + sz

    second = []

    def forward(fd):
        here = slot(fd, 0)
        for gd in (1, 3, 2):
            cp = copy(
                pay.at[here], pay.at[here], g2_s.at[fd, gd - 1], g2_r.at[fd, gd - 1],
                plane_dev(gd * c, gd * (1 - c)),
            )
            cp.start()
            second.append((fd, gd, cp))

    forward(0)
    plane_copies = []
    for i, d in enumerate(plane):
        cp = copy(mplane_own, mplane.at[i], mp_s.at[i], mp_r.at[i], plane_dev(*d))
        cp.start()
        plane_copies.append(cp)
    for fd in (1, 3, 2):
        first[fd - 1].wait_recv()
        forward(fd)
    for cp in w_copies:
        cp.wait()

    lane = lax.broadcasted_iota(jnp.int32, (32, NCH), 1)
    row = lax.broadcasted_iota(jnp.int32, (32, NCH), 0)

    def channelize(gd):
        for fd in range(4):
            n = slot(fd, gd)
            base = fd * 128
            nx = n // 4
            nz = n % 4
            is_first = (((y * 2 + nz % 2) * 4 + nx) * 2 + c) * 2 + nz // 2 == 0
            for part in range(2):
                current = pay[n, part, 8:40, :]
                before = pay[n, part, 7:39, :]
                before = jnp.where(jnp.logical_and(row == 0, is_first), 0.0, before)
                for r in range(4):
                    frame = current if r == 3 else jnp.where(lane < 64 * (r + 1), current, before)
                    high, low = split(frame * win[r : r + 1, :])
                    at_row = base + r * 32
                    at_col = part * 256
                    xs[at_row : at_row + 32, at_col : at_col + 256] = high
                    xs[at_row : at_row + 32, 512 + at_col : 768 + at_col] = low
                    xs[at_row : at_row + 32, 1024 + at_col : 1280 + at_col] = high
        result = jnp.dot(xs[...], wscr[...], preferred_element_type=F32)
        for fd in range(4):
            ysc[slot(fd, gd)] = result[fd * 128 : (fd + 1) * 128]

    channelize(0)

    for cp in plane_copies:
        cp.wait_recv()
    drops = mplane[15]
    for i in range(len(plane)):
        drops = drops + mplane[i]
    slab_lane = lax.broadcasted_iota(jnp.int32, (8, 128), 1)
    slab_row = lax.broadcasted_iota(jnp.int32, (8, 128), 0)
    slab_of_row = ((y * 2 + slab_row % 2) * 4 + slab_row // 2) * 2 + c
    through = jnp.sum(jnp.where(slab_lane <= slab_of_row, drops, 0.0), axis=1, keepdims=True)
    through = through.astype(jnp.int32)
    upper_turn = (((128 + slab_lane) * (through & 255)) & 255).astype(F32) * (2.0 * math.pi / 256)
    ltab[0] = jnp.cos(upper_turn)
    ltab[1] = jnp.sin(upper_turn)
    lower_turn = (((64 * zh + slab_lane) * (through & 255)) & 255).astype(F32) * (2.0 * math.pi / 256)
    pad = jnp.zeros((120, 128), F32)
    ktab[0] = jnp.concatenate([jnp.cos(lower_turn), pad], axis=0).T
    ktab[1] = jnp.concatenate([jnp.sin(lower_turn), pad], axis=0).T
    q_lane = lax.broadcasted_iota(jnp.int32, (16, 128), 1)
    q_row = lax.broadcasted_iota(jnp.int32, (16, 128), 0)
    frame_time = (4 * (q_lane % 32) + q_lane // 32) * HOP
    q_y = (y + q_row // 4) % 4
    q_c = (c + (q_row // 2) % 2) % 2
    q_bin = 2 * (((q_y * 2 + zl) * 4 + x) * 2 + q_c) + q_row % 2
    scale = 1.0 / math.sqrt(Q)
    for i in range(8):
        clock = (frame_time + through[i : i + 1, :]) & (PERIOD - 1)
        turn = ((q_bin * clock) & (PERIOD - 1)).astype(F32) * (2.0 * math.pi / PERIOD)
        etab[i, 0] = jnp.cos(turn) * scale
        etab[i, 1] = jnp.sin(turn) * scale

    k_lane = lax.broadcasted_iota(jnp.int32, (64, 128), 1)

    def finish(n):
        slab = (n // 4) * 2 + n % 2
        lower = ysc[n, :, 0:128].T
        real, imag = lower[0:64], lower[64:128]
        pc = jnp.sum(jnp.where(k_lane == slab, ktab[0, 0:64], 0.0), axis=1, keepdims=True)
        ps = jnp.sum(jnp.where(k_lane == slab, ktab[1, 0:64], 0.0), axis=1, keepdims=True)
        at[n, 0] = real * pc + imag * ps
        at[n, 1] = imag * pc - real * ps
        real, imag = ysc[n, :, 128:256], ysc[n, :, 256:384]
        lc = ltab[0, pl.ds(slab, 1), :]
        ls = ltab[1, pl.ds(slab, 1), :]
        rh, rl = split(real * lc + imag * ls)
        ih, il = split(imag * lc - real * ls)
        for place, (re, im) in enumerate(((rh, ih), (rh, ih), (rl, il))):
            at_row = place * 256
            wb[n, at_row : at_row + 128, 0:128] = re
            wb[n, at_row : at_row + 128, 128:256] = -im
            wb[n, at_row + 128 : at_row + 256, 0:128] = im
            wb[n, at_row + 128 : at_row + 256, 128:256] = re

    def finish_group(gd):
        for fd in range(4):
            finish(slot(fd, gd))

    finish_group(0)
    for gd in (1, 3, 2):
        for fd, g, cp in second:
            if g == gd:
                cp.wait_recv()
        channelize(gd)
        finish_group(gd)

    def stage(bins, acc):
        acc[...] = jnp.zeros_like(acc)

        def step(n, carry):
            slab = (n // 4) * 2 + n % 2
            ar, ai = at[n, 0], at[n, 1]
            rows = []
            for b in bins:
                ec = etab[slab, 0, b : b + 1, :]
                es = etab[slab, 1, b : b + 1, :]
                rh, rl = split(ar * ec + ai * es)
                ih, il = split(ai * ec - ar * es)
                rows.append(jnp.concatenate([rh, ih, rl, il, rh, ih], axis=1))
            left = jnp.concatenate(rows, axis=0)
            found = jnp.dot(left, wb[n], preferred_element_type=F32)
            re, im = found[:, 0:128], found[:, 128:256]
            acc[0] = acc[0] + re
            acc[1] = acc[1] + im
            acc[2] = jnp.maximum(acc[2], re * re + im * im)
            return carry

        lax.fori_loop(0, 16, step, 0)

    partner = dev(y, x, z, (c + 1) % 2)
    partner_copies = []
    ring_copies = []

    def merge(h):
        partner_copies[h].wait_recv()
        acc_o[h, 0] = acc_o[h, 0] + rec_p[h, 0]
        acc_o[h, 1] = acc_o[h, 1] + rec_p[h, 1]
        acc_o[h, 2] = jnp.maximum(acc_o[h, 2], rec_p[h, 2])

    def to_partner(h):
        cp = copy(acc_p.at[h], rec_p.at[h], d_s.at[h], d_r.at[h], partner)
        cp.start()
        partner_copies.append(cp)

    def to_ring(h, half, dy):
        cp = copy(
            acc_o.at[h, :, pl.ds(half * 128, 128), :], rec_y.at[dy - 1], y_s.at[dy - 1],
            y_r.at[dy - 1], dev((y + dy) % 4, x, z, c),
        )
        cp.start()
        ring_copies.append(cp)

    def bins_of(dys, dc):
        return [dy * 4 + dc * 2 + qq for dy in dys for qq in range(2)]

    stage(bins_of((2, 1), 1), acc_p.at[0])
    to_partner(0)
    stage(bins_of((2, 1), 0), acc_o.at[0])
    merge(0)
    to_ring(0, 0, 2)
    to_ring(0, 1, 1)
    stage(bins_of((3, 0), 1), acc_p.at[1])
    to_partner(1)
    stage(bins_of((3, 0), 0), acc_o.at[1])
    merge(1)
    to_ring(1, 0, 3)
    for cp in ring_copies:
        cp.wait_recv()
    mine = slice(128, 256)
    norm = 1.0 / math.sqrt(128.0)
    for part in range(2):
        value = acc_o[1, part, mine] + rec_y[0, part]
        value = value + (rec_y[1, part] + rec_y[2, part])
        out_coh[part] = value * norm
    value = jnp.maximum(acc_o[1, 2, mine], rec_y[0, 2])
    value = jnp.maximum(value, jnp.maximum(rec_y[1, 2], rec_y[2, 2]))
    out_max[...] = jnp.sqrt(value)

    margin.wait_send()
    for cp in team_copies + plane_copies + first + partner_copies + ring_copies:
        cp.wait_send()
    for fd, gd, cp in second:
        cp.wait_send()


def own_slot(device):
    return device["x"] * 4 + device["zh"] * 2 + device["zl"]


def on_device(capture, dropped):
    win, filters = tables()
    slab = ((lax.axis_index("y") * 2 + lax.axis_index("zl")) * 4 + lax.axis_index("x")) * 2
    slab = slab + lax.axis_index("c")
    lanes = lax.broadcasted_iota(jnp.int32, (8, 128), 1)
    counted = jnp.logical_and(lanes == slab, lax.axis_index("zh") == 0)
    meta = jnp.where(counted, dropped[0], 0).astype(F32)
    vmem = pl.BlockSpec(memory_space=pltpu.VMEM)
    dma = pltpu.SemaphoreType.DMA
    held, coherent = pl.pallas_call(
        kernel,
        out_shape=(
            jax.ShapeDtypeStruct((128, 128), F32),
            jax.ShapeDtypeStruct((2, 128, 128), F32),
        ),
        in_specs=[vmem, vmem, vmem, pl.BlockSpec(memory_space=pl.ANY)],
        out_specs=(vmem, vmem),
        scratch_shapes=[
            pltpu.VMEM((16, 2, 40, 256), F32),
            pltpu.VMEM((512, 1536), BF16),
            pltpu.VMEM((1536, 384), BF16),
            pltpu.VMEM((16, 128, 384), F32),
            pltpu.VMEM((16, 2, 64, 128), F32),
            pltpu.VMEM((16, 768, 256), BF16),
            pltpu.VMEM((8, 2, 16, 128), F32),
            pltpu.VMEM((2, 8, 128), F32),
            pltpu.VMEM((2, 128, 128), F32),
            pltpu.VMEM((7, 8, 128), F32),
            pltpu.VMEM((16, 8, 128), F32),
            pltpu.VMEM((2, 3, 256, 128), F32),
            pltpu.VMEM((2, 3, 256, 128), F32),
            pltpu.VMEM((2, 3, 256, 128), F32),
            pltpu.VMEM((3, 3, 128, 128), F32),
            dma((3, 3)), dma, dma, dma((7,)), dma((7,)), dma((15,)), dma((15,)), dma((3,)), dma((3,)),
            dma((4, 3)), dma((4, 3)), dma((2,)), dma((2,)), dma((3,)), dma((3,)),
        ],
        compiler_params=pltpu.CompilerParams(collective_id=0, has_side_effects=True),
    )(capture.reshape(2, 32, 256), meta, jnp.asarray(win), jnp.asarray(filters))
    return held.reshape(2, 64, 128), coherent.reshape(2, 2, 64, 128)


def solution(mesh):
    fine = Mesh(mesh.devices.reshape(4, 2, 4, 2, 2), AXES)
    slabs = ("y", "zl", "x", "c")
    return jax.shard_map(
        on_device,
        mesh=fine,
        in_specs=(P(None, AXES), P(slabs)),
        out_specs=(P(slabs, "zh", None), P(None, slabs, "zh", None)),
        check_vma=False,
    )
```
